32 devices in a mesh: groups: 2 (over y), row: 4 (over z), col: 4 (over x, core).
Axes of the slice: x: 2, y: 2, z: 4, core: 2. Of those that a mesh axis runs over, the one named last changes fastest.
Arguments:
- activations: bfloat16 [768, 4096], P(('groups', 'row'), 'col'), parts along dimension 0, may hold values from -52 to 52
- damping: float32 [8192], P(('groups', 'row')), parts along dimension 0, may hold values from 0.1 to 1
Outputs:
- factor: float32 [8192, 4096], P(('groups', 'row'), 'col'), parts along dimension 0
The draws below stay inside these ranges and needn't reach their ends.
There are 2 independent parts, one for each index of `groups`. The reference program is written for one: setup_inputs(seed, part) draws one part's arguments, and reference() takes and returns one part's arrays. A program takes and returns all parts, laid end to end along the dimension named above; each array names one. Nothing has to cross between parts.
All inputs are finite; a program needn't handle non-finite values.
Results may differ from the reference program's by a relative error of at most 0.0003.
Values may be sent and summed in bfloat16 or wider, within the bound.
A program may use at most 64 MiB of HBM per device.

```python
import math
import jax
import jax.numpy as jnp
from jax import lax

D = 4096
NB = 256
PANELS = 2
TOKENS = 384


def draw_activations(key, part):
    draw_keys = jax.random.split(key, 5)
    row_scale = jnp.exp(jax.random.uniform(draw_keys[0], (TOKENS, 1), jnp.float32, math.log(0.3), math.log(3.0)))
    col_scale = jnp.exp(jax.random.uniform(draw_keys[1], (1, D), jnp.float32, math.log(0.3), math.log(3.0)))
    first_perm = jax.random.permutation(draw_keys[2], D)
    second_perm = jax.random.permutation(draw_keys[3], D)
    base_draw = jnp.clip(jax.random.normal(draw_keys[4], (TOKENS, D), jnp.float32), -4.0, 4.0)
    mixed = base_draw + 0.6 * base_draw[:, first_perm] + 0.4 * base_draw[:, second_perm]
    return (mixed * row_scale * col_scale / 1.4).astype(jnp.bfloat16)


def steps_of(stream_key, shape, cuts, smallest, top_value):
    def one(position, blocks):
        draws = jax.random.uniform(jax.random.fold_in(jax.random.fold_in(stream_key, 6), position), (blocks,), jnp.float32, smallest / len(cuts), top_value / len(cuts))
        return jnp.repeat(jnp.exp(draws), shape[position] // blocks).reshape((-1,) + (1,) * (len(shape) - position - 1))

    level = one(*cuts[0])
    for cut in cuts[1:]:
        level = level * one(*cut)
    return level


def setup_inputs(seed: int = 0, part: int = 0) -> dict:
    key_of = jax.random.split(jax.random.key(seed), 3)
    own_keys = jax.random.split(jax.random.fold_in(key_of[2], part), 3)
    activations = draw_activations(jax.random.fold_in(jax.random.fold_in(key_of[2], part), 71), part)
    damping = jnp.clip(jnp.exp(math.log(1.0) - 2.3025851 * jax.random.uniform(own_keys[1], (D,), jnp.float32) ** steps_of(own_keys[1], (D,), ((0, 4),), -0.2, 0.2)), 0.1, 1.0)
    return {"activations": activations, "damping": damping}


def reference(activations, damping):
    gram = lax.dot_general(activations.astype(jnp.float32), activations.astype(jnp.float32), (((0,), (0,)), ((), ())), preferred_element_type=jnp.float32)
    matrix = gram / TOKENS + jnp.diag(damping)
    for panel_index in range(PANELS):
        begin_at = panel_index * NB
        end_at = begin_at + NB
        pivot_block = jnp.linalg.cholesky(matrix[begin_at:end_at, begin_at:end_at])
        panel_rows = jax.scipy.linalg.solve_triangular(pivot_block, matrix[end_at:, begin_at:end_at].T, lower=True).T
        update = jnp.dot(panel_rows.astype(jnp.float32), panel_rows.T.astype(jnp.float32), precision=lax.Precision.HIGHEST, preferred_element_type=jnp.float32)
        matrix = matrix.at[end_at:, end_at:].add(-update)
        matrix = matrix.at[begin_at:end_at, begin_at:end_at].set(pivot_block)
        matrix = matrix.at[end_at:, begin_at:end_at].set(panel_rows)
        matrix = matrix.at[begin_at:end_at, end_at:].set(0.0)
    return matrix
```

```python
import functools

import jax
import jax.numpy as jnp
from jax import lax
from jax.experimental import pallas as pl
from jax.experimental.pallas import tpu as pltpu
from jax.sharding import PartitionSpec as P

NB = 256
PANELS = 2
LEAD = NB * PANELS
BLK = 128
SUB = 8
HIGHEST = lax.Precision.HIGHEST
MESH = pl.DeviceIdType.MESH


def dot(a, b, dims, precision=None):
    return lax.dot_general(
        a, b, (dims, ((), ())), precision=precision, preferred_element_type=jnp.float32
    )


def split2(x):
    hi = x.astype(jnp.bfloat16)
    lo = (x - hi.astype(jnp.float32)).astype(jnp.bfloat16)
    return hi, lo


def factor_block(s):
    lane = lax.broadcasted_iota(jnp.int32, (SUB, BLK), 1)
    sub = lax.broadcasted_iota(jnp.int32, (SUB, BLK), 0)
    groups = BLK // SUB
    rows = [s[SUB * g : SUB * (g + 1), :] for g in range(groups)]
    upper, inverse = [], []
    for g in range(groups):
        mine = rows[g]
        first = SUB * g
        cols = [
            jnp.broadcast_to(mine[:, first + k : first + k + 1], (SUB, BLK)) for k in range(SUB)
        ]
        diag = jnp.zeros((SUB, BLK), jnp.float32)
        recip = jnp.zeros((SUB, BLK), jnp.float32)
        for j in range(SUB):
            pivot = jnp.broadcast_to(cols[j][j : j + 1, :], (SUB, BLK))
            inv = 1.0 / pivot
            below = sub > j
            at = lane == first + j
            w = jnp.where(below, cols[j] * inv, 0.0)
            diag = jnp.where(sub == j, pivot, diag)
            recip = jnp.where(sub == j, inv, recip)
            for k in range(j + 1, SUB):
                cols[k] = cols[k] - w * jnp.broadcast_to(cols[k][j : j + 1, :], (SUB, BLK))
            row = jnp.where(at, 1.0, jnp.broadcast_to(mine[j : j + 1, :], (SUB, BLK)))
            mine = jnp.where(at & below, 0.0, mine) - w * row
        on = lane == sub + first
        low = lane < sub + first
        inv_part = jnp.where(low, mine, jnp.where(on, 1.0, 0.0))
        root = 1.0 / jnp.sqrt(diag)
        upper.append(jnp.where(low, 0.0, mine) * root)
        inverse.append(inv_part * root)
        if g < groups - 1:
            spread = jnp.where(lane >= first + SUB, mine, inv_part)
            inside = (lane >= first) & (lane < first + SUB)
            weights = (mine * recip).T
            for h in range(g + 1, groups):
                block = weights[SUB * h : SUB * (h + 1), :]
                acc = jnp.where(inside, 0.0, rows[h])
                for j in range(SUB):
                    acc = acc - jnp.broadcast_to(block[:, j : j + 1], (SUB, BLK)) * jnp.broadcast_to(
                        spread[j : j + 1, :], (SUB, BLK)
                    )
                rows[h] = acc
    return jnp.concatenate(upper, 0), jnp.concatenate(inverse, 0)


def gather_kernel(
    nr, nc, a_ref, damp_ref, cols_ref, mir_ref, b_ref, w_ref, l_ref, lead, dlead,
    z_send, z_recv, d_send, d_recv, f_send, f_recv, m_send, m_recv,
):
    local, width = a_ref.shape
    tokens = local * nr
    lw = min(width, LEAD)
    leads = LEAD // lw
    r = lax.axis_index("row")
    c = lax.axis_index("col")
    rest = width - lw

    def rows_of(i):
        return pl.ds(pl.multiple_of(i * local, 16), local)

    barrier = pltpu.get_barrier_semaphore()
    for d in range(1, nr):
        pl.semaphore_signal(
            barrier, inc=1, device_id={"row": lax.rem(r + d, nr)}, device_id_type=MESH
        )
    for d in range(1, nc):
        pl.semaphore_signal(
            barrier, inc=1, device_id={"col": lax.rem(c + d, nc)}, device_id_type=MESH
        )
    pl.semaphore_wait(barrier, nr + nc - 2)

    def z_copy(part, src_row, d):
        span = pl.ds(0, lw) if part == 0 else pl.ds(lw, rest)
        return pltpu.make_async_remote_copy(
            src_ref=a_ref.at[:, span],
            dst_ref=cols_ref.at[rows_of(src_row), span],
            send_sem=z_send.at[part, d],
            recv_sem=z_recv.at[part, src_row],
            device_id={"row": lax.rem(r + d, nr)},
            device_id_type=MESH,
        )

    def d_copy(src_row, d):
        span = pl.ds(pl.multiple_of(src_row * lw, 128), lw)
        return pltpu.make_async_remote_copy(
            src_ref=damp_ref.at[:, pl.ds(0, lw)],
            dst_ref=dlead.at[:, span],
            send_sem=d_send.at[d],
            recv_sem=d_recv.at[src_row],
            device_id={"row": lax.rem(r + d, nr)},
            device_id_type=MESH,
        )

    def f_copy(src_row, src_col, d):
        place = lead.at[rows_of(src_row), pl.ds(pl.multiple_of(src_col * lw, 128), lw)]
        return pltpu.make_async_remote_copy(
            src_ref=cols_ref.at[rows_of(src_row), pl.ds(0, lw)],
            dst_ref=place,
            send_sem=f_send.at[src_row, d],
            recv_sem=f_recv.at[src_col, src_row],
            device_id={"col": lax.rem(c + d, nc)},
            device_id_type=MESH,
        )

    def m_copy(src_row, d):
        return pltpu.make_async_remote_copy(
            src_ref=cols_ref.at[rows_of(src_row), :],
            dst_ref=mir_ref.at[rows_of(src_row), :],
            send_sem=m_send.at[src_row, d],
            recv_sem=m_recv.at[src_row],
            device_id={"col": lax.rem(c + d, nc)},
            device_id_type=MESH,
        )

    parts = 2 if rest else 1
    for d in range(1, nr):
        z_copy(0, r, d).start()

    @pl.when(r < leads)
    def _():
        for d in range(1, nr):
            d_copy(r, d).start()
        dlead[:, pl.ds(pl.multiple_of(jnp.minimum(r, leads - 1) * lw, 128), lw)] = damp_ref[:, :lw]

    cols_ref[rows_of(r), :] = a_ref[...]
    if rest:
        for d in range(1, nr):
            z_copy(1, r, d).start()

    for e in range(1, nr):
        z_copy(0, lax.rem(r + e, nr), e).wait_recv()

        @pl.when(c < leads)
        def _():
            for d in range(1, nc):
                f_copy(lax.rem(r + e, nr), c, d).start()

    @pl.when(c < leads)
    def _():
        for d in range(1, nc):
            f_copy(r, c, d).start()
        lead[:, pl.ds(pl.multiple_of(jnp.minimum(c, leads - 1) * lw, 128), lw)] = cols_ref[:, :lw]

    for src_col in range(leads):

        @pl.when(c != src_col)
        def _():
            for i in range(nr):
                f_copy(i, src_col, 1).wait_recv()

    for src_row in range(leads):

        @pl.when(r != src_row)
        def _():
            d_copy(src_row, 1).wait_recv()

    eye_t = lax.broadcasted_iota(jnp.int32, (tokens, tokens), 0) == lax.broadcasted_iota(
        jnp.int32, (tokens, tokens), 1
    )
    w_ref[...] = jnp.where(eye_t, 1.0 / tokens, 0.0)

    def step(k, carry):
        span = pl.ds(pl.multiple_of(k * BLK, BLK), BLK)
        a_k = lead[:, span].astype(jnp.float32)
        z = dot(w_ref[...], a_k, ((1,), (0,)), HIGHEST)
        eye = lax.broadcasted_iota(jnp.int32, (BLK, BLK), 0) == lax.broadcasted_iota(
            jnp.int32, (BLK, BLK), 1
        )
        s = dot(a_k, z, ((0,), (0,)), HIGHEST) + jnp.where(eye, dlead[:, span], 0.0)
        upper, inverse = factor_block(s)
        l_ref[span, :] = upper.T
        b = dot(inverse, z, ((1,), (1,)), HIGHEST)
        b_ref[span, :] = b
        w_ref[...] = w_ref[...] - dot(b, b, ((0,), (0,)), HIGHEST)
        return carry

    step(0, 0)

    if rest:
        for e in range(1, nr):
            z_copy(1, lax.rem(r + e, nr), e).wait_recv()

    @pl.when(r == c)
    def _():
        for i in range(nr):
            for d in range(1, nc):
                m_copy(i, d).start()
        mir_ref[...] = cols_ref[...]

    lax.fori_loop(1, LEAD // BLK, step, 0)

    @pl.when(r != c)
    def _():
        for i in range(nr):
            m_copy(i, 1).wait_recv()

    @pl.when(r == c)
    def _():
        for i in range(nr):
            for d in range(1, nc):
                m_copy(i, d).wait_send()

    @pl.when(c < leads)
    def _():
        for i in range(nr):
            for d in range(1, nc):
                f_copy(i, c, d).wait_send()

    @pl.when(r < leads)
    def _():
        for d in range(1, nr):
            d_copy(r, d).wait_send()

    for part in range(parts):
        for d in range(1, nr):
            z_copy(part, r, d).wait_send()


def update_kernel(cols_ref, mir_ref, b_ref, w_ref, l_ref, damp_ref, out_ref, y_hi, y_lo):
    tile, width = out_ref.shape
    i = pl.program_id(0)
    r = lax.axis_index("row")
    c = lax.axis_index("col")
    lw = min(width, LEAD)

    @pl.when(i == 0)
    def _():
        hi, lo = split2(w_ref[...])
        y = dot(hi, cols_ref[...], ((1,), (0,))) + dot(lo, cols_ref[...], ((1,), (0,)))
        y_hi[...], y_lo[...] = split2(y)

    a = mir_ref[...]
    s = dot(a, y_hi[...], ((0,), (0,))) + dot(a, y_lo[...], ((0,), (0,)))
    row = i * tile + lax.broadcasted_iota(jnp.int32, (tile, width), 0)
    col = lax.broadcasted_iota(jnp.int32, (tile, width), 1)
    s = s + jnp.where((row == col) & (r == c), damp_ref[...], 0.0)
    out_ref[...] = jnp.where(r * width + row >= LEAD, s, 0.0)

    @pl.when(c * width < LEAD)
    def _():
        base = pl.multiple_of(jnp.minimum(c * width, LEAD - lw), BLK)
        hi, lo = split2(b_ref[pl.ds(base, lw), :])
        p = dot(a, hi, ((0,), (1,))) + dot(a, lo, ((0,), (1,)))
        grow = r * width + i * tile + lax.broadcasted_iota(jnp.int32, (tile, lw), 0)
        gcol = c * width + lax.broadcasted_iota(jnp.int32, (tile, lw), 1)
        out_ref[:, :lw] = jnp.where(grow >= gcol, p, 0.0)
        for t in range(tile // BLK):
            for q in range(lw // BLK):

                @pl.when((r == c) & (i * (tile // BLK) + t == q))
                def _():
                    out_ref[t * BLK : (t + 1) * BLK, q * BLK : (q + 1) * BLK] = l_ref[
                        pl.ds(base + q * BLK, BLK), :
                    ]


def on_device(nr, nc, activations, damping):
    local, width = activations.shape
    tokens = local * nr
    lw = min(width, LEAD)
    leads = LEAD // lw
    damp = damping.reshape(1, width)
    vmem = pl.BlockSpec(memory_space=pltpu.VMEM)
    dma = pltpu.SemaphoreType.DMA
    cols, mir, b, w, l = pl.pallas_call(
        functools.partial(gather_kernel, nr, nc),
        out_shape=(
            jax.ShapeDtypeStruct((tokens, width), jnp.bfloat16),
            jax.ShapeDtypeStruct((tokens, width), jnp.bfloat16),
            jax.ShapeDtypeStruct((LEAD, tokens), jnp.float32),
            jax.ShapeDtypeStruct((tokens, tokens), jnp.float32),
            jax.ShapeDtypeStruct((LEAD, BLK), jnp.float32),
        ),
        in_specs=[vmem] * 2,
        out_specs=(vmem,) * 5,
        scratch_shapes=[
            pltpu.VMEM((tokens, LEAD), jnp.bfloat16),
            pltpu.VMEM((1, LEAD), jnp.float32),
            dma((2, nr)),
            dma((2, nr)),
            dma((nr,)),
            dma((leads,)),
            dma((nr, nc)),
            dma((leads, nr)),
            dma((nr, nc)),
            dma((nr,)),
        ],
        compiler_params=pltpu.CompilerParams(
            collective_id=0, has_side_effects=True, vmem_limit_bytes=60 * 2**20
        ),
        name="gather_factor",
    )(activations, damp)
    tile = min(256, width)
    whole = lambda shape: pl.BlockSpec(shape, lambda i: (0, 0))
    return pl.pallas_call(
        update_kernel,
        grid=(width // tile,),
        out_shape=jax.ShapeDtypeStruct((width, width), jnp.float32),
        in_specs=[
            whole((tokens, width)),
            pl.BlockSpec((tokens, tile), lambda i: (0, i)),
            whole((LEAD, tokens)),
            whole((tokens, tokens)),
            whole((LEAD, BLK)),
            whole((1, width)),
        ],
        out_specs=pl.BlockSpec((tile, width), lambda i: (i, 0)),
        scratch_shapes=[
            pltpu.VMEM((tokens, width), jnp.bfloat16),
            pltpu.VMEM((tokens, width), jnp.bfloat16),
        ],
        compiler_params=pltpu.CompilerParams(vmem_limit_bytes=60 * 2**20),
        name="update",
    )(cols, mir, b, w, l, damp)


def solution(mesh):
    in_specs = (P(("groups", "row"), "col"), P(("groups", "row")))
    out_specs = P(("groups", "row"), "col")
    body = functools.partial(on_device, mesh.shape["row"], mesh.shape["col"])
    return jax.shard_map(
        body, mesh=mesh, in_specs=in_specs, out_specs=out_specs, check_vma=False
    )
```

```python
import functools

import jax
import jax.numpy as jnp
from jax import lax
from jax.experimental import pallas as pl
from jax.experimental.pallas import tpu as pltpu
from jax.sharding import PartitionSpec as P

NB = 256
PANELS = 2
LEAD = NB * PANELS
BLK = 128
SUB = 8
HIGHEST = lax.Precision.HIGHEST
MESH = pl.DeviceIdType.MESH


def dot(a, b, dims, precision=None):
    return lax.dot_general(
        a, b, (dims, ((), ())), precision=precision, preferred_element_type=jnp.float32
    )


def split2(x):
    hi = x.astype(jnp.bfloat16)
    lo = (x - hi.astype(jnp.float32)).astype(jnp.bfloat16)
    return hi, lo


def split3(x):
    hi = x.astype(jnp.bfloat16)
    rest = x - hi.astype(jnp.float32)
    mid = rest.astype(jnp.bfloat16)
    lo = (rest - mid.astype(jnp.float32)).astype(jnp.bfloat16)
    return hi, mid, lo


def dot_pair(x, y, dims):
    (xh, xl), (yh, yl) = x, y
    return dot(xh, yl, dims) + dot(xl, yh, dims) + dot(xh, yh, dims)


def eliminate(s):
    lane = lax.broadcasted_iota(jnp.int32, (SUB, BLK), 1)
    sub = lax.broadcasted_iota(jnp.int32, (SUB, BLK), 0)
    groups = BLK // SUB

    def lanes(x, k):
        return jnp.broadcast_to(x[:, k : k + 1], (SUB, BLK))

    def subs(x, k):
        return jnp.broadcast_to(x[k : k + 1, :], (SUB, BLK))

    rows = [s[SUB * g : SUB * (g + 1), :] for g in range(groups)]
    upper, inverse = [], []
    for g in range(groups):
        mine = rows[g]
        first = SUB * g
        inside = (lane >= first) & (lane < first + SUB)
        more = g + 1 < groups
        cols = [lanes(mine, first + k) for k in range(SUB)]
        if more:
            after = [lanes(rows[g + 1], first + k) for k in range(SUB)]
            follow = jnp.where(inside, 0.0, rows[g + 1])
        diag = jnp.zeros((SUB, BLK), jnp.float32)
        recip = jnp.zeros((SUB, BLK), jnp.float32)
        for j in range(SUB):
            pivot = subs(cols[j], j)
            inv = 1.0 / pivot
            below = sub > j
            at = lane == first + j
            w = jnp.where(below, cols[j], 0.0) * inv
            diag = jnp.where(sub == j, pivot, diag)
            recip = jnp.where(sub == j, inv, recip)
            row = jnp.where(at, 1.0, subs(mine, j))
            row = jnp.where(inside & (lane > first + j), 0.0, row)
            if more:
                v = after[j] * inv
            for k in range(j + 1, SUB):
                head = subs(cols[k], j)
                cols[k] = cols[k] - w * head
                if more:
                    after[k] = after[k] - v * head
            full = jnp.where(at, 1.0, subs(mine, j))
            mine = jnp.where(at & below, 0.0, mine) - w * full
            if more:
                follow = follow - v * row
        on = lane == sub + first
        low = lane < sub + first
        inv_part = jnp.where(low, mine, jnp.where(on, 1.0, 0.0))
        root = lax.rsqrt(diag)
        root = root * (1.5 - 0.5 * diag * root * root)
        upper.append(jnp.where(low, 0.0, mine) * root)
        inverse.append(inv_part * root)
        if more:
            rows[g + 1] = follow
        if g + 2 < groups:
            spread = jnp.where(lane >= first + SUB, mine, inv_part)
            weights = (mine * recip).T
            for h in range(g + 2, groups):
                block = weights[SUB * h : SUB * (h + 1), :]
                acc = jnp.where(inside, 0.0, rows[h])
                for j in range(SUB):
                    acc = acc - jnp.broadcast_to(block[:, j : j + 1], (SUB, BLK)) * subs(spread, j)
                rows[h] = acc
    return jnp.concatenate(upper, 0), jnp.concatenate(inverse, 0)


def factor_step(a_k, damp, w):
    eye = lax.broadcasted_iota(jnp.int32, (BLK, BLK), 0) == lax.broadcasted_iota(
        jnp.int32, (BLK, BLK), 1
    )
    over = ((1,), (0,))
    wh, wm, wl = split3(w)
    z = dot(wl, a_k, over) + dot(wm, a_k, over) + dot(wh, a_k, over)
    zh, zm, zl = split3(z)
    first = ((0,), (0,))
    s = dot(a_k, zl, first) + dot(a_k, zm, first) + dot(a_k, zh, first)
    upper, inverse = eliminate(s + jnp.where(eye, damp, 0.0))
    b = dot_pair(split2(inverse), (zh, zm), ((1,), (1,)))
    bs = split2(b)
    return upper.T, b, w - dot_pair(bs, bs, first)


def gather_kernel(
    nr, nc, a_ref, damp_ref, cols_ref, mir_ref, b_ref, w_ref, l_ref, lead, dlead,
    z_send, z_recv, d_send, d_recv, f_send, f_recv, fp_send, m_send, m_recv, mp_send,
):
    local, width = a_ref.shape
    tokens = local * nr
    lw = min(width, LEAD)
    leads = LEAD // lw
    r = lax.axis_index("row")
    c = lax.axis_index("col")
    rest = width - lw
    chips = nc // 2
    chip = c // 2
    core = lax.rem(c, 2)
    partner = c + 1 - 2 * core
    lead_chips = (leads + 1) // 2
    halves = nr // 2

    def rows_of(i):
        return pl.ds(pl.multiple_of(i * local, 16), local)

    barrier = pltpu.get_barrier_semaphore()
    for d in range(1, nr):
        pl.semaphore_signal(
            barrier, inc=1, device_id={"row": lax.rem(r + d, nr)}, device_id_type=MESH
        )
    for d in range(1, nc):
        pl.semaphore_signal(
            barrier, inc=1, device_id={"col": lax.rem(c + d, nc)}, device_id_type=MESH
        )
    pl.semaphore_wait(barrier, nr + nc - 2)

    def z_copy(part, src_row, d):
        span = pl.ds(0, lw) if part == 0 else pl.ds(lw, rest)
        return pltpu.make_async_remote_copy(
            src_ref=a_ref.at[:, span],
            dst_ref=cols_ref.at[rows_of(src_row), span],
            send_sem=z_send.at[part, d],
            recv_sem=z_recv.at[part, src_row],
            device_id={"row": lax.rem(r + d, nr)},
            device_id_type=MESH,
        )

    def d_copy(src_row, d):
        span = pl.ds(pl.multiple_of(src_row * lw, 128), lw)
        return pltpu.make_async_remote_copy(
            src_ref=damp_ref.at[:, pl.ds(0, lw)],
            dst_ref=dlead.at[:, span],
            send_sem=d_send.at[d],
            recv_sem=d_recv.at[src_row],
            device_id={"row": lax.rem(r + d, nr)},
            device_id_type=MESH,
        )

    def target(i, d):
        there = 2 * lax.rem(chip + d, chips) + lax.rem(i, 2)
        return {"col": partner if d == 0 else there}

    def place(src_row, src_col):
        return lead.at[rows_of(src_row), pl.ds(pl.multiple_of(src_col * lw, 128), lw)]

    def f_copy(src_row, src_col, d):
        return pltpu.make_async_remote_copy(
            src_ref=cols_ref.at[rows_of(src_row), pl.ds(0, lw)],
            dst_ref=place(src_row, src_col),
            send_sem=f_send.at[src_row, d],
            recv_sem=f_recv.at[src_col, src_row],
            device_id=target(src_row, d),
            device_id_type=MESH,
        )

    def fp_copy(src_row, src_col):
        return pltpu.make_async_remote_copy(
            src_ref=place(src_row, src_col),
            dst_ref=place(src_row, src_col),
            send_sem=fp_send.at[src_col, src_row],
            recv_sem=f_recv.at[src_col, src_row],
            device_id={"col": partner},
            device_id_type=MESH,
        )

    def m_copy(src_row, d):
        return pltpu.make_async_remote_copy(
            src_ref=cols_ref.at[rows_of(src_row), :],
            dst_ref=mir_ref.at[rows_of(src_row), :],
            send_sem=m_send.at[src_row, d],
            recv_sem=m_recv.at[src_row],
            device_id=target(src_row, d),
            device_id_type=MESH,
        )

    def mp_copy(src_row):
        return pltpu.make_async_remote_copy(
            src_ref=mir_ref.at[rows_of(src_row), :],
            dst_ref=mir_ref.at[rows_of(src_row), :],
            send_sem=mp_send.at[src_row],
            recv_sem=m_recv.at[src_row],
            device_id={"col": partner},
            device_id_type=MESH,
        )

    def others():
        for part in range(2 if rest else 1):
            for d in range(1, nr):
                z_copy(part, r, d).start()

    @pl.when(c < leads)
    def _():
        for d in range(1, nr):
            z_copy(0, r, d).start()

    @pl.when(chip >= lead_chips)
    def _():
        others()

    @pl.when(r < leads)
    def _():
        for d in range(1, nr):
            d_copy(r, d).start()
        dlead[:, pl.ds(pl.multiple_of(jnp.minimum(r, leads - 1) * lw, 128), lw)] = damp_ref[:, :lw]

    cols_ref[rows_of(r), :] = a_ref[...]

    @pl.when(c < leads)
    def _():
        for e in range(1, nr):
            i = lax.rem(r + e, nr)
            z_copy(0, i, e).wait_recv()
            for d in list(range(1, chips)) + [0]:
                f_copy(i, c, d).start()
        for d in list(range(1, chips)) + [0]:
            f_copy(r, c, d).start()
        if rest:
            for d in range(1, nr):
                z_copy(1, r, d).start()
        lead[:, pl.ds(pl.multiple_of(jnp.minimum(c, leads - 1) * lw, 128), lw)] = cols_ref[:, :lw]

    if lead_chips * 2 > leads:

        @pl.when((c >= leads) & (chip < lead_chips))
        def _():
            f_copy(lax.rem(r + 1, nr), 0, 0).wait_recv()
            others()

    for src_col in range(leads):

        @pl.when((c != src_col) & (chip == src_col // 2))
        def _():
            for e in range(nr):
                i = lax.rem(r + e, nr)
                if src_col == 0 and e == 1:

                    @pl.when(c < leads)
                    def _():
                        f_copy(i, src_col, 0).wait_recv()

                else:
                    f_copy(i, src_col, 0).wait_recv()

        @pl.when(chip != src_col // 2)
        def _():
            for q in range(halves):
                f_copy(2 * q + core, src_col, 0).wait_recv()
                fp_copy(2 * q + core, src_col).start()
            for q in range(halves):
                f_copy(2 * q + 1 - core, src_col, 0).wait_recv()

    for src_row in range(leads):

        @pl.when(r != src_row)
        def _():
            d_copy(src_row, 1).wait_recv()

    eye_t = lax.broadcasted_iota(jnp.int32, (tokens, tokens), 0) == lax.broadcasted_iota(
        jnp.int32, (tokens, tokens), 1
    )
    w_ref[...] = jnp.where(eye_t, 1.0 / tokens, 0.0)

    @pl.loop(0, LEAD // BLK)
    def _(k):
        span = pl.ds(pl.multiple_of(k * BLK, BLK), BLK)
        l, b, w = factor_step(lead[:, span], dlead[:, span], w_ref[...])
        l_ref[span, :] = l
        b_ref[span, :] = b
        w_ref[...] = w

        @pl.when(k == 1)
        def _():
            @pl.when(c < leads)
            def _():
                if rest:
                    for e in range(1, nr):
                        z_copy(1, lax.rem(r + e, nr), e).wait_recv()

            @pl.when(c >= leads)
            def _():
                for part in range(2 if rest else 1):
                    for e in range(1, nr):
                        z_copy(part, lax.rem(r + e, nr), e).wait_recv()

            @pl.when(r == c)
            def _():
                for i in range(nr):
                    for d in list(range(1, chips)) + [0]:
                        m_copy(i, d).start()
                mir_ref[...] = cols_ref[...]

        @pl.when((k == 2) & (chip != r // 2))
        def _():
            for q in range(halves):
                m_copy(2 * q + core, 0).wait_recv()
                mp_copy(2 * q + core).start()

    @pl.when((r != c) & (chip == r // 2))
    def _():
        for i in range(nr):
            m_copy(i, 0).wait_recv()

    @pl.when(chip != r // 2)
    def _():
        for q in range(halves):
            m_copy(2 * q + 1 - core, 0).wait_recv()
            mp_copy(2 * q + core).wait_send()

    @pl.when(r == c)
    def _():
        for i in range(nr):
            for d in range(chips):
                m_copy(i, d).wait_send()

    for src_col in range(leads):

        @pl.when(chip != src_col // 2)
        def _():
            for q in range(halves):
                fp_copy(2 * q + core, src_col).wait_send()

    @pl.when(c < leads)
    def _():
        for i in range(nr):
            for d in range(chips):
                f_copy(i, c, d).wait_send()

    @pl.when(r < leads)
    def _():
        for d in range(1, nr):
            d_copy(r, d).wait_send()

    for part in range(2 if rest else 1):
        for d in range(1, nr):
            z_copy(part, r, d).wait_send()


def update_kernel(cols_ref, mir_ref, b_ref, w_ref, l_ref, damp_ref, out_ref, y_hi, y_lo):
    tile, width = out_ref.shape
    i = pl.program_id(0)
    r = lax.axis_index("row")
    c = lax.axis_index("col")
    lw = min(width, LEAD)

    @pl.when(i == 0)
    def _():
        hi, lo = split2(w_ref[...])
        y = dot(hi, cols_ref[...], ((1,), (0,))) + dot(lo, cols_ref[...], ((1,), (0,)))
        y_hi[...], y_lo[...] = split2(y)

    a = mir_ref[:, pl.ds(pl.multiple_of(i * tile, BLK), tile)]
    s = dot(a, y_hi[...], ((0,), (0,))) + dot(a, y_lo[...], ((0,), (0,)))
    row = i * tile + lax.broadcasted_iota(jnp.int32, (tile, width), 0)
    col = lax.broadcasted_iota(jnp.int32, (tile, width), 1)
    s = s + jnp.where((row == col) & (r == c), damp_ref[...], 0.0)
    out_ref[...] = jnp.where(r * width + row >= LEAD, s, 0.0)

    @pl.when(c * width < LEAD)
    def _():
        base = pl.multiple_of(jnp.minimum(c * width, LEAD - lw), BLK)
        hi, lo = split2(b_ref[pl.ds(base, lw), :])
        p = dot(a, hi, ((0,), (1,))) + dot(a, lo, ((0,), (1,)))
        grow = r * width + i * tile + lax.broadcasted_iota(jnp.int32, (tile, lw), 0)
        gcol = c * width + lax.broadcasted_iota(jnp.int32, (tile, lw), 1)
        out_ref[:, :lw] = jnp.where(grow >= gcol, p, 0.0)
        for t in range(tile // BLK):
            for q in range(lw // BLK):

                @pl.when((r == c) & (i * (tile // BLK) + t == q))
                def _():
                    out_ref[t * BLK : (t + 1) * BLK, q * BLK : (q + 1) * BLK] = l_ref[
                        pl.ds(base + q * BLK, BLK), :
                    ]


def on_device(nr, nc, activations, damping):
    local, width = activations.shape
    tokens = local * nr
    lw = min(width, LEAD)
    leads = LEAD // lw
    damp = damping.reshape(1, width)
    limit = min(60 * 2**20, 16 * 2**20 + 48 * tokens * tokens)
    vmem = pl.BlockSpec(memory_space=pltpu.VMEM)
    dma = pltpu.SemaphoreType.DMA
    cols, mir, b, w, l = pl.pallas_call(
        functools.partial(gather_kernel, nr, nc),
        out_shape=(
            jax.ShapeDtypeStruct((tokens, width), jnp.bfloat16),
            jax.ShapeDtypeStruct((tokens, width), jnp.bfloat16),
            jax.ShapeDtypeStruct((LEAD, tokens), jnp.float32),
            jax.ShapeDtypeStruct((tokens, tokens), jnp.float32),
            jax.ShapeDtypeStruct((LEAD, BLK), jnp.float32),
        ),
        in_specs=[vmem] * 2,
        out_specs=(vmem,) * 5,
        scratch_shapes=[
            pltpu.VMEM((tokens, LEAD), jnp.bfloat16),
            pltpu.VMEM((1, LEAD), jnp.float32),
            dma((2, nr)),
            dma((2, nr)),
            dma((nr,)),
            dma((leads,)),
            dma((nr, nc // 2)),
            dma((leads, nr)),
            dma((leads, nr)),
            dma((nr, nc // 2)),
            dma((nr,)),
            dma((nr,)),
        ],
        compiler_params=pltpu.CompilerParams(
            collective_id=0, has_side_effects=True, vmem_limit_bytes=limit
        ),
        name="gather_factor",
    )(activations, damp)
    tile = min(256, width)
    return pl.pallas_call(
        update_kernel,
        grid=(width // tile,),
        out_shape=jax.ShapeDtypeStruct((width, width), jnp.float32),
        in_specs=[vmem] * 6,
        out_specs=pl.BlockSpec((tile, width), lambda i: (i, 0)),
        scratch_shapes=[
            pltpu.VMEM((tokens, width), jnp.bfloat16),
            pltpu.VMEM((tokens, width), jnp.bfloat16),
        ],
        compiler_params=pltpu.CompilerParams(vmem_limit_bytes=limit),
        name="update",
    )(cols, mir, b, w, l, damp)


def solution(mesh):
    in_specs = (P(("groups", "row"), "col"), P(("groups", "row")))
    out_specs = P(("groups", "row"), "col")
    body = functools.partial(on_device, mesh.shape["row"], mesh.shape["col"])
    return jax.shard_map(
        body, mesh=mesh, in_specs=in_specs, out_specs=out_specs, check_vma=False
    )
```

```python
import functools

import jax
import jax.numpy as jnp
from jax import lax
from jax.experimental import pallas as pl
from jax.experimental.pallas import tpu as pltpu
from jax.sharding import PartitionSpec as P

NB = 256
PANELS = 2
LEAD = NB * PANELS
BLK = 128
SUB = 8
HIGHEST = lax.Precision.HIGHEST
MESH = pl.DeviceIdType.MESH


def dot(a, b, dims, precision=None):
    return lax.dot_general(
        a, b, (dims, ((), ())), precision=precision, preferred_element_type=jnp.float32
    )


def split2(x):
    hi = x.astype(jnp.bfloat16)
    lo = (x - hi.astype(jnp.float32)).astype(jnp.bfloat16)
    return hi, lo


def split3(x):
    hi = x.astype(jnp.bfloat16)
    rest = x - hi.astype(jnp.float32)
    mid = rest.astype(jnp.bfloat16)
    lo = (rest - mid.astype(jnp.float32)).astype(jnp.bfloat16)
    return hi, mid, lo


def dot_pair(x, y, dims):
    (xh, xl), (yh, yl) = x, y
    return dot(xh, yl, dims) + dot(xl, yh, dims) + dot(xh, yh, dims)


def eliminate(s):
    lane = lax.broadcasted_iota(jnp.int32, (SUB, BLK), 1)
    sub = lax.broadcasted_iota(jnp.int32, (SUB, BLK), 0)
    groups = BLK // SUB

    def lanes(x, k):
        return jnp.broadcast_to(x[:, k : k + 1], (SUB, BLK))

    def subs(x, k):
        return jnp.broadcast_to(x[k : k + 1, :], (SUB, BLK))

    rows = [s[SUB * g : SUB * (g + 1), :] for g in range(groups)]
    upper, inverse = [], []
    for g in range(groups):
        mine = rows[g]
        first = SUB * g
        inside = (lane >= first) & (lane < first + SUB)
        more = g + 1 < groups
        cols = [lanes(mine, first + k) for k in range(SUB)]
        if more:
            after = [lanes(rows[g + 1], first + k) for k in range(SUB)]
            follow = jnp.where(inside, 0.0, rows[g + 1])
        diag = jnp.zeros((SUB, BLK), jnp.float32)
        recip = jnp.zeros((SUB, BLK), jnp.float32)
        for j in range(SUB):
            pivot = subs(cols[j], j)
            inv = 1.0 / pivot
            below = sub > j
            at = lane == first + j
            w = jnp.where(below, cols[j], 0.0) * inv
            diag = jnp.where(sub == j, pivot, diag)
            recip = jnp.where(sub == j, inv, recip)
            row = jnp.where(at, 1.0, subs(mine, j))
            row = jnp.where(inside & (lane > first + j), 0.0, row)
            if more:
                v = after[j] * inv
            for k in range(j + 1, SUB):
                head = subs(cols[k], j)
                cols[k] = cols[k] - w * head
                if more:
                    after[k] = after[k] - v * head
            full = jnp.where(at, 1.0, subs(mine, j))
            mine = jnp.where(at & below, 0.0, mine) - w * full
            if more:
                follow = follow - v * row
        on = lane == sub + first
        low = lane < sub + first
        inv_part = jnp.where(low, mine, jnp.where(on, 1.0, 0.0))
        root = lax.rsqrt(diag)
        root = root * (1.5 - 0.5 * diag * root * root)
        upper.append(jnp.where(low, 0.0, mine) * root)
        inverse.append(inv_part * root)
        if more:
            rows[g + 1] = follow
        if g + 2 < groups:
            spread = jnp.where(lane >= first + SUB, mine, inv_part)
            weights = (mine * recip).T
            for h in range(g + 2, groups):
                block = weights[SUB * h : SUB * (h + 1), :]
                acc = jnp.where(inside, 0.0, rows[h])
                for j in range(SUB):
                    acc = acc - jnp.broadcast_to(block[:, j : j + 1], (SUB, BLK)) * subs(spread, j)
                rows[h] = acc
    return jnp.concatenate(upper, 0), jnp.concatenate(inverse, 0)


def factor_step(a_k, damp, w):
    eye = lax.broadcasted_iota(jnp.int32, (BLK, BLK), 0) == lax.broadcasted_iota(
        jnp.int32, (BLK, BLK), 1
    )
    over = ((1,), (0,))
    wh, wm, wl = split3(w)
    z = dot(wl, a_k, over) + dot(wm, a_k, over) + dot(wh, a_k, over)
    zh, zm, zl = split3(z)
    first = ((0,), (0,))
    s = dot(a_k, zl, first) + dot(a_k, zm, first) + dot(a_k, zh, first)
    upper, inverse = eliminate(s + jnp.where(eye, damp, 0.0))
    last = ((1,), (1,))
    bt = dot_pair((zh, zm), split2(inverse), last)
    bs = split2(bt)
    return upper.T, bt, w - dot_pair(bs, bs, last)


def gather_kernel(
    nr, nc, a_hbm, damp_hbm, cols_ref, mir_ref, b_ref, w_ref, l_ref, lead, dlead, damp_ref, load,
    z_send, z_recv, d_send, d_recv, f_send, f_recv, fp_send, m_send, m_recv, mp_send,
):
    local, width = a_hbm.shape
    tokens = local * nr
    lw = min(width, LEAD)
    leads = LEAD // lw
    r = lax.axis_index("row")
    c = lax.axis_index("col")
    rest = width - lw
    chips = nc // 2
    chip = c // 2
    core = lax.rem(c, 2)
    partner = c + 1 - 2 * core
    lead_chips = (leads + 1) // 2
    halves = nr // 2
    every = [0, 1] if rest else [0]

    def rows_of(i):
        return pl.ds(pl.multiple_of(i * local, 16), local)

    bring = pltpu.make_async_copy(a_hbm, cols_ref.at[rows_of(r), :], load.at[0])
    bring_damp = pltpu.make_async_copy(damp_hbm, damp_ref, load.at[1])
    bring.start()
    bring_damp.start()
    barrier = pltpu.get_barrier_semaphore()
    for d in range(1, nr):
        pl.semaphore_signal(
            barrier, inc=1, device_id={"row": lax.rem(r + d, nr)}, device_id_type=MESH
        )
    for d in range(1, nc):
        pl.semaphore_signal(
            barrier, inc=1, device_id={"col": lax.rem(c + d, nc)}, device_id_type=MESH
        )
    pl.semaphore_wait(barrier, nr + nc - 2)
    bring.wait()
    bring_damp.wait()

    def z_copy(part, src_row, d):
        span = pl.ds(0, lw) if part == 0 else pl.ds(lw, rest)
        return pltpu.make_async_remote_copy(
            src_ref=cols_ref.at[rows_of(r), span],
            dst_ref=cols_ref.at[rows_of(src_row), span],
            send_sem=z_send.at[part, d],
            recv_sem=z_recv.at[part, src_row],
            device_id={"row": lax.rem(r + d, nr)},
            device_id_type=MESH,
        )

    def d_copy(src_row, d):
        span = pl.ds(pl.multiple_of(src_row * lw, 128), lw)
        return pltpu.make_async_remote_copy(
            src_ref=damp_ref.at[:, pl.ds(0, lw)],
            dst_ref=dlead.at[:, span],
            send_sem=d_send.at[d],
            recv_sem=d_recv.at[src_row],
            device_id={"row": lax.rem(r + d, nr)},
            device_id_type=MESH,
        )

    def target(i, d):
        there = 2 * lax.rem(chip + d, chips) + lax.rem(i, 2)
        return {"col": partner if d == 0 else there}

    def place(src_row, src_col):
        return lead.at[rows_of(src_row), pl.ds(pl.multiple_of(src_col * lw, 128), lw)]

    def f_copy(src_row, src_col, d):
        return pltpu.make_async_remote_copy(
            src_ref=cols_ref.at[rows_of(src_row), pl.ds(0, lw)],
            dst_ref=place(src_row, src_col),
            send_sem=f_send.at[src_row, d],
            recv_sem=f_recv.at[src_col, src_row],
            device_id=target(src_row, d),
            device_id_type=MESH,
        )

    def fp_copy(src_row, src_col):
        return pltpu.make_async_remote_copy(
            src_ref=place(src_row, src_col),
            dst_ref=place(src_row, src_col),
            send_sem=fp_send.at[src_col, src_row],
            recv_sem=f_recv.at[src_col, src_row],
            device_id={"col": partner},
            device_id_type=MESH,
        )

    def m_copy(src_row, d):
        return pltpu.make_async_remote_copy(
            src_ref=cols_ref.at[rows_of(src_row), :],
            dst_ref=mir_ref.at[rows_of(src_row), :],
            send_sem=m_send.at[src_row, d],
            recv_sem=m_recv.at[src_row],
            device_id=target(src_row, d),
            device_id_type=MESH,
        )

    def mp_copy(src_row):
        return pltpu.make_async_remote_copy(
            src_ref=mir_ref.at[rows_of(src_row), :],
            dst_ref=mir_ref.at[rows_of(src_row), :],
            send_sem=mp_send.at[src_row],
            recv_sem=m_recv.at[src_row],
            device_id={"col": partner},
            device_id_type=MESH,
        )

    def others(parts):
        for part in parts:
            for d in range(nr):
                ahead = lax.rem(c + d - r + nr, nr)

                @pl.when(ahead != 0)
                def _():
                    z_copy(part, r, ahead).start()

    @pl.when(c < leads)
    def _():
        for d in range(1, nr):
            z_copy(0, r, d).start()

    @pl.when(chip >= lead_chips)
    def _():
        others(every)

    @pl.when(r < leads)
    def _():
        for d in range(1, nr):
            d_copy(r, d).start()
        dlead[:, pl.ds(pl.multiple_of(jnp.minimum(r, leads - 1) * lw, 128), lw)] = damp_ref[:, :lw]

    @pl.when(c < leads)
    def _():
        for e in range(1, nr):
            i = lax.rem(r + e, nr)
            z_copy(0, i, e).wait_recv()
            for d in list(range(1, chips)) + [0]:
                f_copy(i, c, d).start()
        for d in list(range(1, chips)) + [0]:
            f_copy(r, c, d).start()
        if rest:
            others([1])
        lead[:, pl.ds(pl.multiple_of(jnp.minimum(c, leads - 1) * lw, 128), lw)] = cols_ref[:, :lw]

    if lead_chips * 2 > leads:

        @pl.when((c >= leads) & (chip < lead_chips))
        def _():
            f_copy(lax.rem(r + 1, nr), 0, 0).wait_recv()
            others(every)

    for src_col in range(leads):

        @pl.when((c != src_col) & (chip == src_col // 2))
        def _():
            for e in range(nr):
                i = lax.rem(r + e, nr)
                if src_col == 0 and e == 1:

                    @pl.when(c < leads)
                    def _():
                        f_copy(i, src_col, 0).wait_recv()

                else:
                    f_copy(i, src_col, 0).wait_recv()

        @pl.when(chip != src_col // 2)
        def _():
            for q in range(halves):
                f_copy(2 * q + core, src_col, 0).wait_recv()
                fp_copy(2 * q + core, src_col).start()
            for q in range(halves):
                f_copy(2 * q + 1 - core, src_col, 0).wait_recv()

    for src_row in range(leads):

        @pl.when(r != src_row)
        def _():
            d_copy(src_row, 1).wait_recv()

    def z_wait():
        @pl.when(c < leads)
        def _():
            if rest:
                for e in range(1, nr):
                    z_copy(1, lax.rem(r + e, nr), e).wait_recv()

        @pl.when(c >= leads)
        def _():
            for part in every:
                for e in range(1, nr):
                    z_copy(part, lax.rem(r + e, nr), e).wait_recv()

    eye_t = lax.broadcasted_iota(jnp.int32, (tokens, tokens), 0) == lax.broadcasted_iota(
        jnp.int32, (tokens, tokens), 1
    )
    w_ref[...] = jnp.where(eye_t, 1.0 / tokens, 0.0)

    @pl.loop(0, LEAD // BLK)
    def _(k):
        span = pl.ds(pl.multiple_of(k * BLK, BLK), BLK)
        l, b, w = factor_step(lead[:, span], dlead[:, span], w_ref[...])
        l_ref[span, :] = l
        b_ref[:, span] = b
        w_ref[...] = w

        @pl.when((k == 0) & (r == c))
        def _():
            z_wait()
            for i in range(nr):
                for d in list(range(1, chips)) + [0]:
                    m_copy(i, d).start()
            mir_ref[...] = cols_ref[...]

        @pl.when((k == 2) & (chip != r // 2))
        def _():
            for q in range(halves):
                m_copy(2 * q + core, 0).wait_recv()
                mp_copy(2 * q + core).start()

    @pl.when(r != c)
    def _():
        z_wait()

    @pl.when((r != c) & (chip == r // 2))
    def _():
        for i in range(nr):
            m_copy(i, 0).wait_recv()

    @pl.when(chip != r // 2)
    def _():
        for q in range(halves):
            m_copy(2 * q + 1 - core, 0).wait_recv()
            mp_copy(2 * q + core).wait_send()

    @pl.when(r == c)
    def _():
        for i in range(nr):
            for d in range(chips):
                m_copy(i, d).wait_send()

    for src_col in range(leads):

        @pl.when(chip != src_col // 2)
        def _():
            for q in range(halves):
                fp_copy(2 * q + core, src_col).wait_send()

    @pl.when(c < leads)
    def _():
        for i in range(nr):
            for d in range(chips):
                f_copy(i, c, d).wait_send()

    @pl.when(r < leads)
    def _():
        for d in range(1, nr):
            d_copy(r, d).wait_send()

    for part in range(2 if rest else 1):
        for d in range(1, nr):
            z_copy(part, r, d).wait_send()


def update_kernel(cols_ref, mir_ref, b_ref, w_ref, l_ref, damp_ref, out_ref, y_hi, y_lo):
    tile, width = out_ref.shape
    i = pl.program_id(0)
    r = lax.axis_index("row")
    c = lax.axis_index("col")
    lw = min(width, LEAD)

    base = pl.multiple_of(jnp.minimum(c * width, LEAD - lw), BLK)

    def fill(span):
        hi, lo = split2(w_ref[...])
        a_c = cols_ref[:, span]
        y = dot(hi, a_c, ((1,), (0,))) + dot(lo, a_c, ((1,), (0,)))
        y_hi[:, span], y_lo[:, span] = split2(y)

    @pl.when((i == 0) & (c * width < LEAD))
    def _():
        y_hi[:, :lw], y_lo[:, :lw] = split2(b_ref[:, pl.ds(base, lw)])

    @pl.when((i == 0) & (c * width >= LEAD))
    def _():
        fill(slice(0, lw))

    if width > lw:

        @pl.when(i == 0)
        def _():
            fill(slice(lw, width))

    a = mir_ref[:, pl.ds(pl.multiple_of(i * tile, BLK), tile)]
    s = dot(a, y_hi[...], ((0,), (0,))) + dot(a, y_lo[...], ((0,), (0,)))
    row = i * tile + lax.broadcasted_iota(jnp.int32, (tile, width), 0)
    col = lax.broadcasted_iota(jnp.int32, (tile, width), 1)
    s = s + jnp.where((row == col) & (r == c), damp_ref[...], 0.0)
    keep = r * width + row >= jnp.minimum(c * width + col, LEAD)
    out_ref[...] = jnp.where(keep, s, 0.0)

    @pl.when(c * width < LEAD)
    def _():
        for t in range(tile // BLK):
            for q in range(lw // BLK):

                @pl.when((r == c) & (i * (tile // BLK) + t == q))
                def _():
                    out_ref[t * BLK : (t + 1) * BLK, q * BLK : (q + 1) * BLK] = l_ref[
                        pl.ds(base + q * BLK, BLK), :
                    ]


def on_device(nr, nc, activations, damping):
    local, width = activations.shape
    tokens = local * nr
    lw = min(width, LEAD)
    leads = LEAD // lw
    damp = damping.reshape(1, width)
    limit = min(60 * 2**20, 16 * 2**20 + 48 * tokens * tokens)
    vmem = pl.BlockSpec(memory_space=pltpu.VMEM)
    dma = pltpu.SemaphoreType.DMA
    cols, mir, b, w, l = pl.pallas_call(
        functools.partial(gather_kernel, nr, nc),
        out_shape=(
            jax.ShapeDtypeStruct((tokens, width), jnp.bfloat16),
            jax.ShapeDtypeStruct((tokens, width), jnp.bfloat16),
            jax.ShapeDtypeStruct((tokens, LEAD), jnp.float32),
            jax.ShapeDtypeStruct((tokens, tokens), jnp.float32),
            jax.ShapeDtypeStruct((LEAD, BLK), jnp.float32),
        ),
        in_specs=[pl.BlockSpec(memory_space=pltpu.HBM)] * 2,
        out_specs=(vmem,) * 5,
        scratch_shapes=[
            pltpu.VMEM((tokens, LEAD), jnp.bfloat16),
            pltpu.VMEM((1, LEAD), jnp.float32),
            pltpu.VMEM((1, width), jnp.float32),
            dma((2,)),
            dma((2, nr)),
            dma((2, nr)),
            dma((nr,)),
            dma((leads,)),
            dma((nr, nc // 2)),
            dma((leads, nr)),
            dma((leads, nr)),
            dma((nr, nc // 2)),
            dma((nr,)),
            dma((nr,)),
        ],
        compiler_params=pltpu.CompilerParams(
            collective_id=0, has_side_effects=True, vmem_limit_bytes=limit
        ),
        name="gather_factor",
    )(activations, damp)
    tile = min(256, width)
    return pl.pallas_call(
        update_kernel,
        grid=(width // tile,),
        out_shape=jax.ShapeDtypeStruct((width, width), jnp.float32),
        in_specs=[vmem] * 6,
        out_specs=pl.BlockSpec((tile, width), lambda i: (i, 0)),
        scratch_shapes=[
            pltpu.VMEM((tokens, width), jnp.bfloat16),
            pltpu.VMEM((tokens, width), jnp.bfloat16),
        ],
        compiler_params=pltpu.CompilerParams(vmem_limit_bytes=limit),
        name="update",
    )(cols, mir, b, w, l, damp)


def solution(mesh):
    in_specs = (P(("groups", "row"), "col"), P(("groups", "row")))
    out_specs = P(("groups", "row"), "col")
    body = functools.partial(on_device, mesh.shape["row"], mesh.shape["col"])
    return jax.shard_map(
        body, mesh=mesh, in_specs=in_specs, out_specs=out_specs, check_vma=False
    )
```
